128 devices in a mesh: rep: 2 (over core), dp: 64 (over x, y, z).
Axes of the slice: x: 4, y: 4, z: 4, core: 2. Of those that a mesh axis runs over, the one named last changes fastest.
Arguments:
- x: bfloat16 [128, 2048, 1024], P(('rep', 'dp')), parts along dimension 0
- dy: bfloat16 [128, 2048, 1024], P(('rep', 'dp')), parts along dimension 0
- w_gate: bfloat16 [2, 1024, 3200], replicated
- w_up: bfloat16 [2, 1024, 3200], replicated
- w_down: bfloat16 [2, 3200, 1024], replicated
- m_w_gate: float32 [2, 1024, 3200], P(None, 'dp')
- m_w_up: float32 [2, 1024, 3200], P(None, 'dp')
- m_w_down: float32 [2, 3200, 1024], P(None, 'dp')
- v_w_gate: float32 [2, 1024, 3200], P(None, 'dp')
- v_w_up: float32 [2, 1024, 3200], P(None, 'dp')
- v_w_down: float32 [2, 3200, 1024], P(None, 'dp')
Outputs:
- output 1: bfloat16 [4, 1024, 3200], P('rep'), parts along dimension 0
- output 2: bfloat16 [4, 1024, 3200], P('rep'), parts along dimension 0
- output 3: bfloat16 [4, 3200, 1024], P('rep'), parts along dimension 0
- output 4: float32 [4, 1024, 3200], P('rep', 'dp'), parts along dimension 0
- output 5: float32 [4, 1024, 3200], P('rep', 'dp'), parts along dimension 0
- output 6: float32 [4, 3200, 1024], P('rep', 'dp'), parts along dimension 0
- output 7: float32 [4, 1024, 3200], P('rep', 'dp'), parts along dimension 0
- output 8: float32 [4, 1024, 3200], P('rep', 'dp'), parts along dimension 0
- output 9: float32 [4, 3200, 1024], P('rep', 'dp'), parts along dimension 0
There are 2 independent parts. The reference program is written for one: setup_inputs(seed, part) draws one part's arguments, and reference() takes and returns one part's arrays. A program takes and returns all parts, laid end to end along the dimension named above; an argument that names none is the same for every part.
All inputs are finite; a program needn't handle non-finite values.
Results may differ from the reference program's by a relative error of at most 0.022.
Values are sent between devices in bfloat16 or wider.
A program may use at most 1.5 GiB of HBM per device.

```python
import jax
import jax.numpy as jnp
from jax import lax

SEQUENCES = 64
TOKENS = 2048
D = 1024
FF = 3200
LAYERS = 2
NAMES = ("w_gate", "w_up", "w_down")
SHAPES = {"w_gate": (LAYERS, D, FF), "w_up": (LAYERS, D, FF), "w_down": (LAYERS, FF, D)}


def bump(key, n, height):
    away = (jnp.arange(n, dtype=jnp.int32) - jax.random.randint(key, (), 0, n, jnp.int32)) % n
    return jnp.where(away < n // 8, height, 1.0)


def together(key, own, strength):
    shared = jax.random.normal(key, own.shape[1:], jnp.float32)
    return (own + strength * shared) * lax.rsqrt(1 + strength * strength)


def setup_inputs(seed: int = 0, part: int = 0) -> dict:
    kx, kdy, ka, kb, kz, kf, kh, kl, *keys = jax.random.split(jax.random.key(seed), 8 + 3 * len(NAMES))
    kx, kdy, ka, kb = (jax.random.fold_in(k, part) for k in (kx, kdy, ka, kb))
    kw, km, kv = (keys[i::3] for i in range(3))
    shape = (SEQUENCES, TOKENS, D)
    much_x, much_dy = jax.random.uniform(kz, (2,), jnp.float32, 0.0, 1.0)
    loud = 2.0 ** jax.random.uniform(jax.random.fold_in(kz, 1), (), jnp.float32, -1.0, 2.0)
    layers = 2.0 ** jax.random.uniform(kl, (LAYERS, 1, 1), jnp.float32, -1.0, 1.0)
    x = together(ka, jax.random.normal(kx, shape, jnp.float32), much_x) * bump(kf, D, 4.0)
    dy = together(kb, jax.random.normal(kdy, shape, jnp.float32), much_dy)
    drawn = {"x": x.astype(jnp.bfloat16), "dy": (loud * dy * (SEQUENCES * TOKENS) ** -0.5).astype(jnp.bfloat16)}
    for key, name in zip(kw, NAMES, strict=True):
        w = jax.random.normal(key, SHAPES[name], jnp.float32) * SHAPES[name][1] ** -0.5
        drawn[name] = (w * {"w_gate": 1.0, "w_up": bump(kh, FF, 4.0), "w_down": layers}[name]).astype(jnp.bfloat16)
    for key, name in zip(km, NAMES, strict=True):
        drawn[f"m_{name}"] = 0.1 * jax.random.normal(key, SHAPES[name], jnp.float32)
    for key, name in zip(kv, NAMES, strict=True):
        drawn[f"v_{name}"] = loud * loud * jax.random.uniform(key, SHAPES[name], jnp.float32, 0.05, 0.15)
    return drawn


def matmul(a, w):
    return jnp.dot(a, w, preferred_element_type=jnp.float32).astype(jnp.bfloat16)


def normed(h):
    wide = h.astype(jnp.float32)
    scale = lax.rsqrt(jnp.mean(wide**2, -1, keepdims=True) + 1e-6)
    return (wide * scale).astype(jnp.bfloat16)


def layer(h, w):
    a = normed(h)
    gate = jnp.dot(a, w["w_gate"], preferred_element_type=jnp.float32)
    up = jnp.dot(a, w["w_up"], preferred_element_type=jnp.float32)
    return h + matmul((jax.nn.silu(gate) * up).astype(jnp.bfloat16), w["w_down"])


def adamw(w, m, v, g):
    m = 0.9 * m + 0.1 * g
    v = 0.95 * v + 0.05 * g * g
    step = m * lax.rsqrt(v + 1e-8) + 0.1 * w
    return (w - 0.02 * step).astype(jnp.bfloat16), m, v


def stack(weights, h):
    return lax.scan(lambda h, w: (layer(h, w), None), h, weights)[0]


def reference(x, dy, w_gate, w_up, w_down, m_w_gate, m_w_up, m_w_down, v_w_gate, v_w_up, v_w_down):
    weights = dict(zip(NAMES, (w_gate, w_up, w_down), strict=True))

    def take(so_far, sequence):
        h, by_y = sequence
        _, back = jax.vjp(lambda w: stack(w, h), weights)
        return jax.tree.map(lambda total, term: total + term.astype(jnp.float32), so_far, back(by_y)[0]), None

    none_yet = {name: jnp.zeros(w.shape, jnp.float32) for name, w in weights.items()}
    by_weights, _ = lax.scan(take, none_yet, (x, dy))
    gradients = [by_weights[name].astype(jnp.bfloat16).astype(jnp.float32) for name in NAMES]
    new = [
        adamw(w.astype(jnp.float32), m, v, g)
        for w, m, v, g in zip((w_gate, w_up, w_down), (m_w_gate, m_w_up, m_w_down), (v_w_gate, v_w_up, v_w_down), gradients, strict=True)
    ]
    return tuple(one[which] for which in range(3) for one in new)
```

```python
import functools

import jax
import jax.numpy as jnp
from jax import lax
from jax.experimental import pallas as pl
from jax.experimental.pallas import tpu as pltpu
from jax.sharding import PartitionSpec as P

NAMES = ("w_gate", "w_up", "w_down")
MESH = pl.DeviceIdType.MESH
BF, F32 = jnp.bfloat16, jnp.float32
TOKENS, D, FF = 2048, 1024, 3200
STRIDE = (16, 4, 1)
ORDER = ((1, 2, 0), (2, 0, 1), (0, 1, 2))
CUTS = ((0, 768), (768, 768), (1536, 768), (2304, 896))
CHUNKS = len(CUTS)
DOWN = D // CHUNKS


def mod4(v):
    return lax.rem(v + 8, 4)


class Net:
    def __init__(self, send_sems, recv_sems):
        self.me = lax.axis_index("dp")
        self.at = (lax.div(self.me, 16), lax.rem(lax.div(self.me, 4), 4), lax.rem(self.me, 4))
        self.send_sems, self.recv_sems = send_sems, recv_sems
        self.used = 0
        self.sent = []

    def device(self, dim, off):
        return self.me + (mod4(self.at[dim] + off) - self.at[dim]) * STRIDE[dim]

    def greet(self):
        barrier = pltpu.get_barrier_semaphore()
        for dim in range(3):
            for off in (1, 2, 3):
                pl.semaphore_signal(barrier, inc=1, device_id={"dp": self.device(dim, off)}, device_id_type=MESH)
        pl.semaphore_wait(barrier, 9)

    def send(self, src, dst, dim, off):
        n = self.used
        self.used += 1
        copy = pltpu.make_async_remote_copy(
            src_ref=src, dst_ref=dst, send_sem=self.send_sems.at[n], recv_sem=self.recv_sems.at[n],
            device_id={"dp": self.device(dim, off)}, device_id_type=MESH,
        )
        copy.start()
        self.sent.append(copy)
        return copy

    def finish(self):
        for copy in self.sent:
            copy.wait_send()
        self.sent = []


def slab(ref, axis, c):
    return ref.at[(slice(None),) * axis + (c,)]


def blocks(shape):
    lead, rows = shape[:-2], shape[-2]
    if rows == 200:
        inner = [(pl.ds(r, 40), slice(None)) for r in range(0, 200, 40)]
    else:
        inner = [(slice(None), slice(None))]
    if len(lead) == 2:
        return lead[0], lambda i: [(i, j) + tail for j in range(lead[1]) for tail in inner]
    if len(lead) == 1:
        return lead[0], lambda i: [(i,) + tail for tail in inner]
    return 1, lambda i: inner


def add_into(dst, *refs):
    trips, cover = blocks(dst.shape)

    def body(i, _):
        for where in cover(i):
            total = refs[0][where].astype(F32)
            for ref in refs[1:]:
                total = total + ref[where].astype(F32)
            dst[where] = total.astype(dst.dtype)
        return 0

    if trips == 1:
        body(0, 0)
    else:
        lax.fori_loop(0, trips, body, 0)


def scatter_buffers(which, width):
    if which < 2:
        g, a, b, c = (4, 4, 4, 16, width), (4, 4, 16, width), (4, 16, width), (16, width)
    else:
        g, a, b, c = (4, 4, 200, width), (4, 200, width), (200, width), (50, width)
    shapes = [g] + [a] * 3 + [b] * 3 + [c] * 3
    scratch = [pltpu.VMEM(s, BF) for s in shapes]
    if which == 2:
        scratch += [pltpu.VMEM((200, width), F32), pltpu.VMEM((4, 50, width), BF)]
    return scratch


SCATTER_SENDS = 9


class Scatter:
    def __init__(self, net, which, chunk, refs):
        self.net, self.which = net, which
        self.g, (self.a1, self.a2, self.a3), (self.b1, self.b2, self.b3), self.c = refs[0], refs[1:4], refs[4:7], refs[7:10]
        if which == 2:
            self.wide, self.cut = refs[10:12]
        self.dims = ORDER[which]
        self.axes = ((1, 1), (2, 0), (0, 0))[which]
        self.way = 1 if (chunk + which) % 2 == 0 else -1

    def start_a(self):
        dim, p, s = self.dims[0], self.net.at[self.dims[0]], self.way
        cut = lambda c: slab(self.g, self.axes[0], mod4(c))
        self.far = self.net.send(cut(p + 2), self.a1, dim, s)
        self.near = self.net.send(cut(p - s), self.a2, dim, -s)

    def mid_a(self):
        dim, p, s = self.dims[0], self.net.at[self.dims[0]], self.way
        self.far.wait_recv()
        add_into(self.a1, self.a1, slab(self.g, self.axes[0], mod4(p + s)))
        self.both = self.net.send(self.a1, self.a3, dim, s)

    def end_a(self):
        p = self.net.at[self.dims[0]]
        self.near.wait_recv()
        self.both.wait_recv()
        add_into(self.a2, self.a2, self.a3, slab(self.g, self.axes[0], p))
        dim, p, s = self.dims[1], self.net.at[self.dims[1]], self.way
        cut = lambda c: slab(self.a2, self.axes[1], mod4(c))
        self.far = self.net.send(cut(p + 2), self.b1, dim, s)
        self.near = self.net.send(cut(p - s), self.b2, dim, -s)

    def mid_b(self):
        dim, p, s = self.dims[1], self.net.at[self.dims[1]], self.way
        self.far.wait_recv()
        add_into(self.b1, self.b1, slab(self.a2, self.axes[1], mod4(p + s)))
        self.both = self.net.send(self.b1, self.b3, dim, s)

    def end_b(self):
        p = self.net.at[self.dims[1]]
        self.near.wait_recv()
        self.both.wait_recv()
        mine = slab(self.a2, self.axes[1], p)
        if self.which < 2:
            self.cut = self.b2
            add_into(self.b2, self.b2, self.b3, mine)
        else:
            add_into(self.wide, self.b2, self.b3, mine)
            for j in range(4):
                self.cut[j] = self.wide[50 * j : 50 * j + 50, :].astype(BF)
        dim, p = self.dims[2], self.net.at[self.dims[2]]
        self.last = [self.net.send(self.cut.at[mod4(p + off)], self.c[off - 1], dim, off) for off in (1, 2, 3)]

    def end_c(self):
        p = self.net.at[self.dims[2]]
        total = self.cut[p].astype(F32)
        for copy, ref in zip(self.last, self.c, strict=True):
            copy.wait_recv()
            total = total + ref[...].astype(F32)
        return total.astype(BF).astype(F32)


def adamw(w, m, v, g):
    m = 0.9 * m + 0.1 * g
    v = 0.95 * v + 0.05 * g * g
    step = m * lax.rsqrt(v + 1e-8) + 0.1 * w
    return (w - 0.02 * step).astype(BF), m, v


GATHER_SENDS = 9


class Gather:
    def __init__(self, net, which, chunk, out, small=None, wide=None):
        self.net, self.which, self.out, self.small, self.wide = net, which, out, small, wide
        self.dims = ORDER[which][::-1]
        self.way = 1 if (chunk + which) % 2 == 0 else -1

    def view(self, fixed):
        dims = (0, 1, 2) if self.which < 2 else (0, 1)
        where = [fixed.get(d, slice(None)) for d in dims]
        while where and isinstance(where[-1], slice):
            where.pop()
        return self.out.at[tuple(where)] if where else self.out

    def start(self, mine):
        x, y, z = self.net.at
        if self.which < 2:
            block = self.view({0: x, 1: y, 2: z})
        else:
            block = self.small.at[z]
        block[...] = mine
        self.first = [self.net.send(block, block, self.dims[0], off) for off in (1, 2, 3)]

    def _both(self, fixed, dim):
        part = self.view(fixed)
        return [self.net.send(part, part, dim, off) for off in (self.way, -self.way)]

    def _on(self, fixed, dim):
        part = self.view({**fixed, dim: mod4(self.net.at[dim] - self.way)})
        return self.net.send(part, part, dim, self.way)

    def second(self):
        for copy in self.first:
            copy.wait_recv()
        at = self.net.at
        a, b, c = ORDER[self.which]
        if self.which == 2:
            for j in range(4):
                self.wide[50 * j : 50 * j + 50, :] = self.small[j].astype(F32)
            row = self.view({0: at[0], 1: at[1]})
            row[...] = self.wide[...].astype(BF)
        self.pair = self._both({a: at[a], b: at[b]}, b)

    def second_on(self):
        at = self.net.at
        a, b, _ = ORDER[self.which]
        self.pair[0].wait_recv()
        self.pair[1].wait_recv()
        self.passed = self._on({a: at[a]}, b)

    def third(self):
        at = self.net.at
        a = ORDER[self.which][0]
        self.passed.wait_recv()
        self.pair = self._both({a: at[a]}, a)

    def third_on(self):
        a = ORDER[self.which][0]
        self.pair[0].wait_recv()
        self.pair[1].wait_recv()
        self.passed = self._on({}, a)

    def last(self):
        self.passed.wait_recv()


def ticks(stages):
    return [(s, t - s) for t in range(CHUNKS + stages - 1) for s in range(stages) if 0 <= t - s < CHUNKS]


def width(which, chunk):
    return CUTS[chunk][1] if which < 2 else DOWN


def columns(which, chunk):
    return pl.ds(*CUTS[chunk]) if which < 2 else pl.ds(DOWN * chunk, DOWN)


def split(refs, counts):
    out, at = [], 0
    for n in counts:
        out.append(refs[at : at + n])
        at += n
    return out


SCATTER_REFS = (10, 10, 12)


def scatter_kernel(*refs):
    grads, ws, ms, vs, w_out, m_out, v_out, rest = split(refs, (3, 3, 3, 3, 3, 3, 3, len(refs) - 21))
    send_sems, recv_sems, load_sems = rest[-3:]
    parts = split(rest[:-3], SCATTER_REFS * CHUNKS)
    net = Net(send_sems, recv_sems)
    net.greet()
    units = [[Scatter(net, which, k, parts[3 * k + which]) for which in range(3)] for k in range(CHUNKS)]
    loads = [
        [
            pltpu.make_async_copy(grads[which].at[..., columns(which, k)], units[k][which].g, load_sems.at[3 * k + which])
            for which in range(3)
        ]
        for k in range(CHUNKS)
    ]
    for chunk in loads:
        for copy in chunk:
            copy.start()
    for stage, k in ticks(6):
        for which in range(3):
            unit = units[k][which]
            if stage == 0:
                loads[k][which].wait()
                unit.start_a()
            elif stage < 5:
                (unit.mid_a, unit.end_a, unit.mid_b, unit.end_b)[stage - 1]()
            else:
                cols = columns(which, k)
                w, m, v = adamw(ws[which][:, cols].astype(F32), ms[which][:, cols], vs[which][:, cols], unit.end_c())
                w_out[which][:, cols] = w
                m_out[which][:, cols] = m
                v_out[which][:, cols] = v
    net.finish()


def scatter_step(grads, w, m, v, ident):
    small = [(16, FF), (16, FF), (50, D)]
    n = SCATTER_SENDS * 3 * CHUNKS
    scratch = [s for k in range(CHUNKS) for which in range(3) for s in scatter_buffers(which, width(which, k))]
    vmem = pl.BlockSpec(memory_space=pltpu.VMEM)
    out = pl.pallas_call(
        scatter_kernel,
        out_shape=[jax.ShapeDtypeStruct(s, t) for t in (BF, F32, F32) for s in small],
        in_specs=[pl.BlockSpec(memory_space=pl.ANY)] * 3 + [vmem] * 9,
        out_specs=[vmem] * 9,
        scratch_shapes=scratch
        + [pltpu.SemaphoreType.DMA((n,)), pltpu.SemaphoreType.DMA((n,)), pltpu.SemaphoreType.DMA((3 * CHUNKS,))],
        compiler_params=pltpu.CompilerParams(collective_id=ident, has_side_effects=True, vmem_limit_bytes=60 * 2**20),
        name=f"scatter_{ident}",
    )(*grads, *w, *m, *v)
    return out[:3], out[3:6], out[6:]


def gather_buffers(which, width):
    if which < 2:
        return [pltpu.VMEM((4, 4, 4, 16, width), BF)]
    return [pltpu.VMEM((4, 4, 200, width), BF), pltpu.VMEM((4, 50, width), BF), pltpu.VMEM((200, width), F32)]


def gather_kernel(*refs):
    ws, outs, rest = split(refs, (3, 3, len(refs) - 6))
    send_sems, recv_sems, store_sems = rest[-3:]
    parts = split(rest[:-3], (1, 1, 3) * CHUNKS)
    net = Net(send_sems, recv_sems)
    net.greet()
    units = [[Gather(net, which, k, *parts[3 * k + which]) for which in range(3)] for k in range(CHUNKS)]
    stores = []
    for stage, k in ticks(6):
        for which in range(3):
            unit = units[k][which]
            if stage == 0:
                unit.start(ws[which][:, columns(which, k)])
            else:
                (unit.second, unit.second_on, unit.third, unit.third_on, unit.last)[stage - 1]()
            if stage == 5:
                copy = pltpu.make_async_copy(unit.out, outs[which].at[..., columns(which, k)], store_sems.at[3 * k + which])
                copy.start()
                stores.append(copy)
    for copy in stores:
        copy.wait()
    net.finish()


def gather_step(w, ident):
    n = GATHER_SENDS * 3 * CHUNKS
    scratch = [s for k in range(CHUNKS) for which in range(3) for s in gather_buffers(which, width(which, k))]
    return pl.pallas_call(
        gather_kernel,
        out_shape=[jax.ShapeDtypeStruct(s, BF) for s in [(4, 4, 4, 16, FF)] * 2 + [(4, 4, 200, D)]],
        in_specs=[pl.BlockSpec(memory_space=pltpu.VMEM)] * 3,
        out_specs=[pl.BlockSpec(memory_space=pl.ANY)] * 3,
        scratch_shapes=scratch
        + [pltpu.SemaphoreType.DMA((n,)), pltpu.SemaphoreType.DMA((n,)), pltpu.SemaphoreType.DMA((3 * CHUNKS,))],
        compiler_params=pltpu.CompilerParams(collective_id=ident, has_side_effects=True, vmem_limit_bytes=60 * 2**20),
        name=f"gather_{ident}",
    )(*w)


def matmul(a, w):
    return jnp.dot(a, w, preferred_element_type=F32).astype(BF)


def normed(h):
    wide = h.astype(F32)
    scale = lax.rsqrt(jnp.mean(wide**2, -1, keepdims=True) + 1e-6)
    return (wide * scale).astype(BF)


def layer(h, w):
    a = normed(h)
    gate = jnp.dot(a, w[0], preferred_element_type=F32)
    up = jnp.dot(a, w[1], preferred_element_type=F32)
    return h + matmul((jax.nn.silu(gate) * up).astype(BF), w[2])


def solution(mesh):
    def step(x, dy, *arrays):
        weights, ms, vs = arrays[:3], arrays[3:6], arrays[6:]
        x, dy = x[0], dy[0]
        me = lax.axis_index("dp")

        def run(per_layer):
            h = x
            for w in per_layer:
                h = layer(h, w)
            return h

        layers = weights[0].shape[0]
        _, back = jax.vjp(run, [[w[number] for w in weights] for number in range(layers)])
        grads = back(dy)[0]
        rows = (16, 16, 50)
        new = [None] * layers
        full = [None] * layers
        for number in reversed(range(layers)):
            g = [grads[number][i].reshape(s) for i, s in enumerate([(4, 4, 4, 16, FF)] * 2 + [(4, 4, 200, D)])]
            w = [lax.dynamic_slice_in_dim(weights[i][number], me * rows[i], rows[i], 0) for i in range(3)]
            new[number] = scatter_step(g, w, [m[number] for m in ms], [v[number] for v in vs], 2 * number)
            full[number] = gather_step(new[number][0], 2 * number + 1)
        w = [jnp.stack([full[number][i].reshape(weights[i].shape[1:]) for number in range(layers)]) for i in range(3)]
        m, v = ([jnp.stack([new[number][which][i] for number in range(layers)]) for i in range(3)] for which in (1, 2))
        return (*w, *m, *v)

    tokens = P(("rep", "dp"))
    return jax.shard_map(
        step,
        mesh=mesh,
        in_specs=(tokens, tokens) + (P(),) * 3 + (P(None, "dp"),) * 6,
        out_specs=(P("rep"),) * 3 + (P("rep", "dp"),) * 6,
        check_vma=False,
    )
```
